32 devices in a mesh: panel: 16 (over z, y, x), lag: 2 (over core).
Axes of the slice: x: 2, y: 2, z: 4, core: 2. Of those that a mesh axis runs over, the one named last changes fastest.
Arguments:
- history: bfloat16 [2, 32, 512, 128], P('lag', 'panel'), may hold values from -6 to 6
- weights: bfloat16 [16, 2, 6, 512, 512], P('panel', 'lag'), may hold values from -0.25 to 0.25
- pairs: int32 [16, 2, 6, 3], P('panel', 'lag'), may hold values from 0 to 4, as said below
- counts: int32 [16, 2], P('panel', 'lag'), may hold values from 3 to 6, as said below
- send_list: int32 [16, 2, 5, 2], P(None, 'lag'), may hold values from 0 to 1
- incident: bfloat16 [32, 512, 128], P(('panel', 'lag')), may hold values from -6 to 6
- near_inverse: bfloat16 [32, 512, 512], P(('panel', 'lag')), may hold values from -0.25 to 0.25
Outputs:
- density: bfloat16 [32, 512, 128], P(('panel', 'lag'))
The draws below stay inside these ranges and needn't reach their ends.
Inputs may be any that keep to these rules, and one draw needn't show every extreme that they name: pairs[p, g, k] = (o, c, r) with o in 0 to 4, c in 0 to 1, r in 0 to 1; the (o, c) of one device's pairs are distinct. `counts`: panel index 0 at lag index 0 has 6 pairs.
All inputs are finite; a program needn't handle non-finite values.
Results may differ from the reference program's by a relative error of at most 0.0083.
Values may be sent and summed in bfloat16 or wider, within the bound.
A program may use at most 64 MiB of HBM per device.

```python
import jax
import jax.numpy as jnp
from jax import lax

PB = 512
RHS = 128
PAIRS_DEV = 6
REACH = 2
CAP = 2
BLK_DEV = 2
LAGS = 2
NBLK = 32
N_PANEL = 16


def draw_pairs(key, part):
    offsets = 2 * REACH + 1
    scores = jax.random.randint(jax.random.fold_in(key, 11), (N_PANEL, LAGS, offsets), 0, 1 << 20) * offsets + jnp.arange(offsets, dtype=jnp.int32)
    order = jnp.argsort(scores, axis=-1, stable=True).astype(jnp.int32)
    position = jnp.arange(PAIRS_DEV, dtype=jnp.int32)
    chosen = jnp.take(order, position // CAP, axis=2)
    slot_index = jnp.broadcast_to(position % CAP, (N_PANEL, LAGS, PAIRS_DEV)).astype(jnp.int32)
    reader = jax.random.randint(jax.random.fold_in(key, 12), (N_PANEL, LAGS, PAIRS_DEV), 0, BLK_DEV).astype(jnp.int32)
    return jnp.stack([chosen, slot_index, reader], axis=-1).astype(jnp.int32)


def draw_counts(key, part):
    extra = jax.random.randint(jax.random.fold_in(key, 21), (N_PANEL, LAGS), 0, 4)
    active = jnp.minimum(3 + extra, PAIRS_DEV)
    return active.at[0, 0].set(PAIRS_DEV).astype(jnp.int32)


def with_ends(values, own_key, smallest, high):
    longest = values.shape.index(max(values.shape))
    spots = []
    for shift in (0, 1):
        where = [jax.random.randint(jax.random.fold_in(own_key, axis), (), 0, length) for axis, length in enumerate(values.shape)]
        where[longest] = (where[longest] + shift) % values.shape[longest]
        spots.append(tuple(where))
    return values.at[spots[0]].set(smallest).at[spots[1]].set(high)


def levels(own_key, dims, pieces, least, high):
    loudness = 1.0
    for axis_at, blocks in pieces:
        heights = jax.random.uniform(jax.random.fold_in(jax.random.fold_in(own_key, 6), axis_at), (blocks,), jnp.float32, least / len(pieces), high / len(pieces))
        loudness = loudness * jnp.repeat(jnp.exp(heights), dims[axis_at] // blocks).reshape((-1,) + (1,) * (len(dims) - 1 - axis_at))
    return loudness


def centred(own_key, shape, scale, limit, split=(), kind=jnp.bfloat16):
    gain = levels(own_key, shape, split, -0.22, 0.18) if split else 1.0
    entries = jax.random.normal(own_key, shape, jnp.float32) * scale * gain
    return jnp.minimum(jnp.maximum(entries, -limit), limit).astype(kind)


def setup_inputs(seed: int = 0) -> dict:
    key_list = jax.random.split(jax.random.key(seed), 8)
    history = centred(key_list[0], (LAGS, NBLK, PB, RHS), 1.0, 6.0, ((0, 2), (1, 16)))
    weights = centred(key_list[1], (N_PANEL, LAGS, PAIRS_DEV, PB, PB), PB ** -0.5, 0.25, ((0, 16), (1, 2)))
    pairs = draw_pairs(jax.random.fold_in(key_list[7], 71), 0)
    counts = draw_counts(jax.random.fold_in(key_list[7], 71), 0)
    send_list = with_ends(jax.random.randint(key_list[4], (N_PANEL, LAGS, 2 * REACH + 1, CAP), 0, BLK_DEV), jax.random.fold_in(key_list[4], 1), 0, BLK_DEV - 1).astype(jnp.int32)
    incident = centred(key_list[5], (NBLK, PB, RHS), 1.0, 6.0, ((0, 32),))
    near_inverse = centred(key_list[6], (NBLK, PB, PB), PB ** -0.5, 0.25, ((0, 32),))
    return dict(history=history, weights=weights, pairs=pairs, counts=counts, send_list=send_list, incident=incident, near_inverse=near_inverse)


def reference(history, weights, pairs, counts, send_list, incident, near_inverse):
    summed = jnp.zeros((NBLK, PB, RHS), jnp.float32)

    def per_device(device, summed):
        panel_idx = (device // LAGS).astype(jnp.int32)
        lag_idx = (device % LAGS).astype(jnp.int32)

        def add_pair(pair_index, summed):
            offset = pairs[panel_idx, lag_idx, pair_index, 0]
            slot_index = pairs[panel_idx, lag_idx, pair_index, 1]
            reader = pairs[panel_idx, lag_idx, pair_index, 2]
            source_panel = ((panel_idx + offset - REACH) % N_PANEL).astype(jnp.int32)
            local_block = send_list[source_panel, lag_idx, offset, slot_index]
            source = history[lag_idx, source_panel * BLK_DEV + local_block]
            product = jnp.dot(weights[panel_idx, lag_idx, pair_index], source, preferred_element_type=jnp.float32)
            target = (panel_idx * BLK_DEV + reader).astype(jnp.int32)
            current = lax.dynamic_index_in_dim(summed, target, 0, keepdims=False)
            return lax.dynamic_update_index_in_dim(summed, current + product, target, 0)

        return lax.fori_loop(0, counts[panel_idx, lag_idx], add_pair, summed)

    summed = lax.fori_loop(0, N_PANEL * LAGS, per_device, summed)
    remainder = (incident.astype(jnp.float32) - summed).astype(jnp.bfloat16)
    density = jnp.einsum("bij,bjr->bir", near_inverse.astype(jnp.float32), remainder.astype(jnp.float32))
    return density.astype(jnp.bfloat16)
```

```python
import functools

import jax
import jax.numpy as jnp
from jax import lax
from jax.experimental import pallas as pl
from jax.experimental.pallas import tpu as pltpu
from jax.sharding import PartitionSpec as P

CHUNKS = 2


def step_kernel(
    relay, panels, lags,
    pairs_ref, counts_ref, send_ref, local_ref, weights_ref, incident_ref, near_ref,
    out_ref,
    window, weights, near, incident, right, partial_value, landed,
    send_sem, recv_sem, local_sem, weight_sem, near_sem, incident_sem,
    sum_send_sem, sum_recv_sem,
):
    here = lax.axis_index("panel")
    lag = lax.axis_index("lag")
    offsets = send_ref.shape[1]
    reach = offsets // 2
    blocks, depth, fields = window.shape[1:]
    count = weights.shape[0]
    own = incident.shape[0]
    side = 2 * lax.rem(here, 2) - 1

    def panel(steps):
        return lax.rem(here + steps + panels, panels)

    def outgoing(steps):
        return local_ref.at[reach - steps] if not relay else window.at[0]

    source_here = local_ref.at[0] if relay else local_ref.at[reach]
    local = pltpu.make_async_copy(source_here, window.at[0], local_sem)
    local.start()
    weight_copies = [
        pltpu.make_async_copy(weights_ref.at[0, 0, k], weights.at[k], weight_sem.at[k])
        for k in range(count)
    ]

    barrier = pltpu.get_barrier_semaphore()
    greeted = [-side, 2 * side, -2 * side] + ([] if relay else [side])
    for steps in greeted:
        pl.semaphore_signal(
            barrier, inc=1, device_id={"panel": panel(steps)},
            device_id_type=pl.DeviceIdType.MESH,
        )
    for ahead in range(1, lags):
        pl.semaphore_signal(
            barrier, inc=1, device_id={"lag": lax.rem(lag + ahead, lags)},
            device_id_type=pl.DeviceIdType.MESH,
        )
    pl.semaphore_wait(barrier, len(greeted) + lags - 1)
    local.wait()

    def send(source, slot, block, steps):
        return pltpu.make_async_remote_copy(
            src_ref=source.at[block],
            dst_ref=window.at[slot, block],
            send_sem=send_sem.at[slot - 1, block],
            recv_sem=recv_sem.at[slot - 1, block],
            device_id={"panel": panel(steps)},
            device_id_type=pl.DeviceIdType.MESH,
        )

    first, second, partner, passed = [], [], [], []
    for block in range(blocks):
        first.append(send(outgoing(2 * side), 3, block, 2 * side))
        partner.append(send(outgoing(-side), 4, block, -side))
        first[-1].start()
        partner[-1].start()
    for block in range(blocks):
        second.append(send(outgoing(-2 * side), 2, block, -2 * side))
        second[-1].start()
    near_copy = pltpu.make_async_copy(near_ref, near, near_sem)
    incident_copy = pltpu.make_async_copy(incident_ref, incident, incident_sem)
    for copy in weight_copies:
        copy.start()
    incident_copy.start()
    near_copy.start()
    for block in range(blocks):
        if relay:
            first[block].wait_recv()
            passed.append(send(window.at[3], 1, block, -side))
        else:
            passed.append(send(outgoing(side), 1, block, side))
        passed[-1].start()
    for copy in weight_copies:
        copy.wait()
    incident_copy.wait()
    near_copy.wait()
    for block in range(blocks):
        if not relay:
            first[block].wait_recv()
        partner[block].wait_recv()
        second[block].wait_recv()
        passed[block].wait_recv()

    live = counts_ref[0, 0]
    readers = right.shape[1] // fields
    for k in range(count):
        offset = pairs_ref[0, 0, 0, k]
        slot = pairs_ref[0, 1, 0, k]
        reader = pairs_ref[0, 2, 0, k]
        if relay:
            block = send_ref[0, offset, slot, panel(offset - reach)]
        else:
            block = slot
        place = lax.rem((offset - reach) * side + offsets, offsets)
        value = window[place, block]
        for r in range(readers):
            kept = jnp.logical_and(reader == r, k < live)
            right[k * depth:(k + 1) * depth, r * fields:(r + 1) * fields] = jnp.where(
                kept, value, jnp.zeros_like(value)
            )

    rows = depth // CHUNKS
    sums = []
    for chunk in range(CHUNKS):
        at = slice(chunk * rows, (chunk + 1) * rows)
        total = None
        for k in range(count):
            term = jnp.dot(
                weights[k, at, :], right[k * depth:(k + 1) * depth, :],
                preferred_element_type=jnp.float32,
            )
            total = term if total is None else total + term
        for r in range(readers):
            partial_value[r, at, :] = total[:, r * fields:(r + 1) * fields]
        for ahead in range(1, lags):
            other = lax.rem(lag + ahead, lags)
            copy = pltpu.make_async_remote_copy(
                src_ref=partial_value.at[pl.ds(other * own, own), pl.ds(chunk * rows, rows)],
                dst_ref=landed.at[ahead - 1, :, pl.ds(chunk * rows, rows)],
                send_sem=sum_send_sem.at[ahead - 1, chunk],
                recv_sem=sum_recv_sem.at[ahead - 1, chunk],
                device_id={"lag": other},
                device_id_type=pl.DeviceIdType.MESH,
            )
            copy.start()
            sums.append(copy)
    for copy in first + partner + second + passed:
        copy.wait_send()
    for copy in sums:
        copy.wait_recv()
    for j in range(own):
        summed = partial_value[lag * own + j]
        for ahead in range(1, lags):
            summed = summed + landed[ahead - 1, j]
        remainder = (incident[j].astype(jnp.float32) - summed).astype(jnp.bfloat16)
        out_ref[j] = jnp.dot(
            near[j], remainder, preferred_element_type=jnp.float32
        ).astype(out_ref.dtype)
    for copy in sums:
        copy.wait_send()


def on_device(panels, lags, history, weights, pairs, counts, send_list, incident, near_inverse):
    readers, depth, fields = history.shape[1:]
    offsets, slots = send_list.shape[2:]
    assert offsets == 5 and panels % 2 == 0 and panels > offsets
    count = weights.shape[2]
    own = incident.shape[0]
    relay = readers <= slots
    blocks = readers if relay else slots
    local = history
    if not relay:
        here = lax.axis_index("panel")
        mine = lax.dynamic_index_in_dim(send_list, here, 0, keepdims=False)[0]
        local = jnp.take(history[0], mine.reshape(-1), axis=0).reshape(
            (offsets, slots, depth, fields)
        )
    anywhere = pl.BlockSpec(memory_space=pl.ANY)
    scalars = pl.BlockSpec(memory_space=pltpu.SMEM)
    dma = pltpu.SemaphoreType.DMA
    return pl.pallas_call(
        functools.partial(step_kernel, relay, panels, lags),
        out_shape=jax.ShapeDtypeStruct(incident.shape, jnp.bfloat16),
        in_specs=[scalars] * 3 + [anywhere] * 4,
        out_specs=pl.BlockSpec(memory_space=pltpu.VMEM),
        scratch_shapes=[
            pltpu.VMEM((offsets, blocks, depth, fields), history.dtype),
            pltpu.VMEM(weights.shape[2:], weights.dtype),
            pltpu.VMEM(near_inverse.shape, near_inverse.dtype),
            pltpu.VMEM(incident.shape, incident.dtype),
            pltpu.VMEM((count * depth, readers * fields), history.dtype),
            pltpu.VMEM((readers, depth, fields), jnp.float32),
            pltpu.VMEM((lags - 1, own, depth, fields), jnp.float32),
            dma((offsets - 1, blocks)),
            dma((offsets - 1, blocks)),
            dma,
            dma((count,)),
            dma,
            dma,
            dma((lags - 1, CHUNKS)),
            dma((lags - 1, CHUNKS)),
        ],
        compiler_params=pltpu.CompilerParams(
            collective_id=0, has_side_effects=True, vmem_limit_bytes=67043328
        ),
    )(jnp.transpose(pairs, (0, 3, 1, 2)), counts, jnp.transpose(send_list, (1, 2, 3, 0)), local, weights, incident, near_inverse)


def solution(mesh):
    return jax.shard_map(
        functools.partial(on_device, mesh.shape["panel"], mesh.shape["lag"]),
        mesh=mesh,
        in_specs=(
            P("lag", "panel", None, None),
            P("panel", "lag", None, None, None),
            P("panel", "lag", None, None),
            P("panel", "lag"),
            P(None, "lag", None, None),
            P(("panel", "lag"), None, None),
            P(("panel", "lag"), None, None),
        ),
        out_specs=P(("panel", "lag"), None, None),
        check_vma=False,
    )
```

```python
import functools

import jax
import jax.numpy as jnp
from jax import lax
from jax.experimental import pallas as pl
from jax.experimental.pallas import tpu as pltpu
from jax.sharding import PartitionSpec as P

CHUNKS = 2
PARTS = 4


def step_kernel(
    relay, panels, lags,
    pairs_ref, counts_ref, send_ref, local_ref, weights_ref, incident_ref, near_ref,
    out_ref,
    windows, weights, near, incident, right, running, partial_value, landed,
    send_sem, recv_sem, local_sem, weight_sem, near_sem, incident_sem,
    sum_send_sem, sum_recv_sem,
):
    here = lax.axis_index("panel")
    lag = lax.axis_index("lag")
    offsets = send_ref.shape[1]
    reach = offsets // 2
    blocks, piece, fields = windows[0].shape[1:]
    depth = piece * PARTS
    count = weights.shape[0]
    own = incident.shape[0]
    side = 2 * lax.rem(here, 2) - 1

    def panel(steps):
        return lax.rem(here + steps + panels, panels)

    def rows_of(part):
        return pl.ds(part * piece, piece)

    def outgoing(steps, part):
        if relay:
            return windows[part].at[0]
        return local_ref.at[reach - steps, :, rows_of(part)]

    source_here = local_ref.at[0] if relay else local_ref.at[reach]
    locals_here = [
        pltpu.make_async_copy(
            source_here.at[:, rows_of(part)], windows[part].at[0], local_sem.at[part]
        )
        for part in range(PARTS)
    ]
    for copy in locals_here:
        copy.start()
    weight_copies = [
        pltpu.make_async_copy(weights_ref.at[0, 0, k], weights.at[k], weight_sem.at[k])
        for k in range(count)
    ]

    barrier = pltpu.get_barrier_semaphore()
    greeted = [-side, 2 * side, -2 * side] + ([] if relay else [side])
    for steps in greeted:
        pl.semaphore_signal(
            barrier, inc=1, device_id={"panel": panel(steps)},
            device_id_type=pl.DeviceIdType.MESH,
        )
    for ahead in range(1, lags):
        pl.semaphore_signal(
            barrier, inc=1, device_id={"lag": lax.rem(lag + ahead, lags)},
            device_id_type=pl.DeviceIdType.MESH,
        )
    pl.semaphore_wait(barrier, len(greeted) + lags - 1)
    for copy in locals_here:
        copy.wait()

    def send(source, slot, part, steps):
        copy = pltpu.make_async_remote_copy(
            src_ref=source,
            dst_ref=windows[part].at[slot],
            send_sem=send_sem.at[slot - 1, part],
            recv_sem=recv_sem.at[slot - 1, part],
            device_id={"panel": panel(steps)},
            device_id_type=pl.DeviceIdType.MESH,
        )
        copy.start()
        return copy

    first, second, partner, passed = [], [], [], []
    lead = PARTS // 2
    for step in range(PARTS + lead):
        if step < PARTS:
            first.append(send(outgoing(2 * side, step), 3, step, 2 * side))
            partner.append(send(outgoing(-side, step), 4, step, -side))
        if step >= lead:
            part = step - lead
            second.append(send(outgoing(-2 * side, part), 2, part, -2 * side))
    near_copy = pltpu.make_async_copy(near_ref, near, near_sem)
    incident_copy = pltpu.make_async_copy(incident_ref, incident, incident_sem)
    for copy in weight_copies:
        copy.start()
    incident_copy.start()
    near_copy.start()
    def pass_on(part):
        if relay:
            first[part].wait_recv()
            passed.append(send(windows[part].at[3], 1, part, -side))
        else:
            passed.append(send(outgoing(side, part), 1, part, side))

    for part in range(PARTS):
        pass_on(part)
    for copy in weight_copies:
        copy.wait()
    incident_copy.wait()
    near_copy.wait()

    live = counts_ref[0, 0]
    readers = right.shape[2] // fields
    chosen = []
    for k in range(count):
        offset = pairs_ref[0, 0, 0, k]
        slot = pairs_ref[0, 1, 0, k]
        reader = pairs_ref[0, 2, 0, k]
        if relay:
            block = send_ref[0, offset, slot, panel(offset - reach)]
        else:
            block = slot
        place = lax.rem((offset - reach) * side + offsets, offsets)
        chosen.append((place, block, reader))

    def arrive(part):
        if not relay:
            first[part].wait_recv()
        partner[part].wait_recv()
        second[part].wait_recv()
        passed[part].wait_recv()
        for k, (place, block, reader) in enumerate(chosen):
            value = windows[part][place, block]
            for r in range(readers):
                kept = jnp.logical_and(reader == r, k < live)
                right[part, k * piece:(k + 1) * piece, r * fields:(r + 1) * fields] = jnp.where(
                    kept, value, jnp.zeros_like(value)
                )

    def product(part, at):
        left = jnp.concatenate(
            [weights[k, at, part * piece:(part + 1) * piece] for k in range(count)], axis=1
        )
        return jnp.dot(left, right[part], preferred_element_type=jnp.float32)

    rows = depth // CHUNKS
    sums = []
    for part in range(PARTS - 1):
        arrive(part)
        for chunk in range(CHUNKS):
            at = slice(chunk * rows, (chunk + 1) * rows)
            term = product(part, at)
            running[at, :] = term if part == 0 else running[at, :] + term
    arrive(PARTS - 1)
    for chunk in range(CHUNKS):
        at = slice(chunk * rows, (chunk + 1) * rows)
        total = running[at, :] + product(PARTS - 1, at)
        for r in range(readers):
            partial_value[r, at, :] = total[:, r * fields:(r + 1) * fields]
        for ahead in range(1, lags):
            other = lax.rem(lag + ahead, lags)
            copy = pltpu.make_async_remote_copy(
                src_ref=partial_value.at[pl.ds(other * own, own), pl.ds(chunk * rows, rows)],
                dst_ref=landed.at[ahead - 1, :, pl.ds(chunk * rows, rows)],
                send_sem=sum_send_sem.at[ahead - 1, chunk],
                recv_sem=sum_recv_sem.at[ahead - 1, chunk],
                device_id={"lag": other},
                device_id_type=pl.DeviceIdType.MESH,
            )
            copy.start()
            sums.append(copy)
    for copy in first + partner + second + passed:
        copy.wait_send()
    for copy in sums:
        copy.wait_recv()
    for j in range(own):
        summed = partial_value[lag * own + j]
        for ahead in range(1, lags):
            summed = summed + landed[ahead - 1, j]
        remainder = (incident[j].astype(jnp.float32) - summed).astype(jnp.bfloat16)
        out_ref[j] = jnp.dot(
            near[j], remainder, preferred_element_type=jnp.float32
        ).astype(out_ref.dtype)
    for copy in sums:
        copy.wait_send()


def on_device(panels, lags, history, weights, pairs, counts, send_list, incident, near_inverse):
    readers, depth, fields = history.shape[1:]
    offsets, slots = send_list.shape[2:]
    assert offsets == 5 and panels % 2 == 0 and panels > offsets
    count = weights.shape[2]
    own = incident.shape[0]
    relay = readers <= slots
    blocks = readers if relay else slots
    local = history
    if not relay:
        here = lax.axis_index("panel")
        mine = lax.dynamic_index_in_dim(send_list, here, 0, keepdims=False)[0]
        local = jnp.take(history[0], mine.reshape(-1), axis=0).reshape(
            (offsets, slots, depth, fields)
        )
    anywhere = pl.BlockSpec(memory_space=pl.ANY)
    scalars = pl.BlockSpec(memory_space=pltpu.SMEM)
    dma = pltpu.SemaphoreType.DMA
    return pl.pallas_call(
        functools.partial(step_kernel, relay, panels, lags),
        out_shape=jax.ShapeDtypeStruct(incident.shape, jnp.bfloat16),
        in_specs=[scalars] * 3 + [anywhere] * 4,
        out_specs=pl.BlockSpec(memory_space=pltpu.VMEM),
        scratch_shapes=[
            [pltpu.VMEM((offsets, blocks, depth // PARTS, fields), history.dtype)] * PARTS,
            pltpu.VMEM(weights.shape[2:], weights.dtype),
            pltpu.VMEM(near_inverse.shape, near_inverse.dtype),
            pltpu.VMEM(incident.shape, incident.dtype),
            pltpu.VMEM((PARTS, count * depth // PARTS, readers * fields), history.dtype),
            pltpu.VMEM((depth, readers * fields), jnp.float32),
            pltpu.VMEM((readers, depth, fields), jnp.float32),
            pltpu.VMEM((lags - 1, own, depth, fields), jnp.float32),
            dma((offsets - 1, PARTS)),
            dma((offsets - 1, PARTS)),
            dma((PARTS,)),
            dma((count,)),
            dma,
            dma,
            dma((lags - 1, CHUNKS)),
            dma((lags - 1, CHUNKS)),
        ],
        compiler_params=pltpu.CompilerParams(
            collective_id=0, has_side_effects=True, vmem_limit_bytes=67043328
        ),
    )(jnp.transpose(pairs, (0, 3, 1, 2)), counts, jnp.transpose(send_list, (1, 2, 3, 0)), local, weights, incident, near_inverse)


def solution(mesh):
    return jax.shard_map(
        functools.partial(on_device, mesh.shape["panel"], mesh.shape["lag"]),
        mesh=mesh,
        in_specs=(
            P("lag", "panel", None, None),
            P("panel", "lag", None, None, None),
            P("panel", "lag", None, None),
            P("panel", "lag"),
            P(None, "lag", None, None),
            P(("panel", "lag"), None, None),
            P(("panel", "lag"), None, None),
        ),
        out_specs=P(("panel", "lag"), None, None),
        check_vma=False,
    )
```
